32 devices in a mesh: prow: 4 (over z), pcol: 8 (over y, x, core).
Axes of the slice: x: 2, y: 2, z: 4, core: 2. Of those that a mesh axis runs over, the one named last changes fastest.
Arguments:
- tiles: bfloat16 [4, 8, 32, 256, 256], P('prow', 'pcol')
- tile_brow: int32 [4, 8, 32], P('prow', 'pcol'), may hold values from 0 to 31, as said below
- tile_bcol: int32 [4, 8, 32], P('prow', 'pcol'), may hold values from 0 to 15, as said below
- tile_count: int32 [4, 8], P('prow', 'pcol'), may hold values from 8 to 32, as said below
Outputs:
- row_scale: float32 [32, 4, 256], P(None, 'prow')
- col_scale: float32 [16, 8, 256], P(None, 'pcol')
The draws below stay inside these ranges and needn't reach their ends.
Inputs may be any that keep to these rules, and one draw needn't show every extreme that they name: `tile_brow`: on one device, no two slots name the same pair of local block row and column; the diagonal tile of every block row is present and live, in the first slots of the device that holds it. `tile_bcol`: see tile_brow. `tile_count`: a device that holds diagonal tiles has all 32 slots live, every other device at most 16.
All inputs are finite; a program needn't handle non-finite values.
Results may differ from the reference program's by a relative error of at most 0.0003.
Values sent between devices are 32-bit elements; how exact they have to be, the bound alone decides.
A program may use at most 64 MiB of HBM per device.

```python
import jax
import jax.numpy as jnp
from jax import lax

TILE = 256
BR_DEV = 32
TILES_DEV = 32
SWEEPS = 3
BC_DEV = 16
N_PROW = 4
N_PCOL = 8


def draw_tiles(key, part):
    shape = (N_PROW, N_PCOL, TILES_DEV, TILE, TILE)
    base = jax.random.normal(jax.random.fold_in(key, 11), shape, jnp.float32)
    span = 2.3
    row_log = jax.random.uniform(jax.random.fold_in(key, 12), (N_PROW, N_PCOL, TILES_DEV, TILE, 1), jnp.float32, -span, span)
    col_log = jax.random.uniform(jax.random.fold_in(key, 13), (N_PROW, N_PCOL, TILES_DEV, 1, TILE), jnp.float32, -span, span)
    return (base * jnp.exp(row_log) * jnp.exp(col_log)).astype(jnp.bfloat16)


def place_slots(key):
    cells = BR_DEV * BC_DEV
    keys = jax.random.split(jax.random.fold_in(key, 21), N_PROW * N_PCOL)
    cell_ids = jnp.arange(cells, dtype=jnp.int32)
    rows_of = cell_ids // BC_DEV
    cols_of = cell_ids % BC_DEV

    def one_device(device_key, position):
        prow_id = position // N_PCOL
        pcol_id = position % N_PCOL
        diagonal = rows_of * N_PROW + prow_id == cols_of * N_PCOL + pcol_id
        order = jax.random.permutation(device_key, cells).astype(jnp.int32)
        score = jnp.where(diagonal, order - cells, order)
        chosen = jnp.argsort(score, stable=True)[:TILES_DEV].astype(jnp.int32)
        return (rows_of[chosen], cols_of[chosen])
    brows, bcols = jax.vmap(one_device)(keys, jnp.arange(N_PROW * N_PCOL, dtype=jnp.int32))
    return (brows.reshape(N_PROW, N_PCOL, TILES_DEV), bcols.reshape(N_PROW, N_PCOL, TILES_DEV))


def draw_tile_brow(key, part):
    return place_slots(key)[0].astype(jnp.int32)


def draw_tile_bcol(key, part):
    return place_slots(key)[1].astype(jnp.int32)


def draw_tile_count(key, part):
    low = max(TILES_DEV // 4, 1)
    high = max(TILES_DEV // 2, low)
    counts = jax.random.randint(jax.random.fold_in(key, 31), (N_PROW, N_PCOL), low, high + 1)
    prow_ids = jnp.arange(N_PROW, dtype=jnp.int32)[:, None]
    pcol_ids = jnp.arange(N_PCOL, dtype=jnp.int32)[None, :]
    holder = pcol_ids % N_PROW == prow_ids
    return jnp.where(holder, TILES_DEV, counts).astype(jnp.int32)


def setup_inputs(seed: int = 0) -> dict:
    key_list = jax.random.split(jax.random.key(seed), 5)
    return {
        "tiles": draw_tiles(jax.random.fold_in(key_list[4], 71), 0),
        "tile_brow": draw_tile_brow(jax.random.fold_in(key_list[4], 71), 0),
        "tile_bcol": draw_tile_bcol(jax.random.fold_in(key_list[4], 71), 0),
        "tile_count": draw_tile_count(jax.random.fold_in(key_list[4], 71), 0),
    }


def rescale(scale, largest):
    return scale / jnp.sqrt(largest)

def reference(tiles, tile_brow, tile_bcol, tile_count):
    live = (jnp.arange(TILES_DEV, dtype=jnp.int32)[None, None, :] < tile_count[:, :, None]).astype(jnp.float32)
    row_vec = jnp.ones((N_PROW, BR_DEV, TILE), jnp.float32)
    col_vec = jnp.ones((N_PCOL, BC_DEV, TILE), jnp.float32)
    col_ids = jnp.arange(N_PCOL, dtype=jnp.int32)[:, None]
    for sweep in range(SWEEPS):

        def one_row(inputs):
            block, brow, bcol, alive, rows = inputs
            row_take = rows[brow]
            col_take = col_vec[col_ids, bcol]
            scaled = jnp.abs(block.astype(jnp.float32)) * row_take[:, :, :, None] * col_take[:, :, None, :]
            row_part = lax.optimization_barrier(jnp.max(scaled, axis=3)) * alive[:, :, None]
            col_part = lax.optimization_barrier(jnp.max(scaled, axis=2)) * alive[:, :, None]
            row_new = jnp.zeros((BR_DEV, TILE), jnp.float32).at[brow.reshape(-1)].max(row_part.reshape(-1, TILE))
            col_new = jnp.zeros((N_PCOL, BC_DEV, TILE), jnp.float32).at[jnp.broadcast_to(col_ids, bcol.shape).reshape(-1), bcol.reshape(-1)].max(col_part.reshape(-1, TILE))
            return (row_new, col_new)
        row_max, col_parts = lax.map(one_row, (tiles, tile_brow, tile_bcol, live, row_vec))
        col_max = lax.optimization_barrier(jnp.max(col_parts, axis=0))
        row_vec = rescale(row_vec, row_max)
        col_vec = rescale(col_vec, col_max)
    return (jnp.transpose(row_vec, (1, 0, 2)), jnp.transpose(col_vec, (1, 0, 2)))
```

```python
import functools

import jax
import jax.numpy as jnp
from jax import lax
from jax.experimental import pallas as pl
from jax.experimental.pallas import tpu as pltpu
from jax.sharding import PartitionSpec as P

BR_DEV = 32
SWEEPS = 3
LANES = 128
STEP = 4
ROWS = 16


def rescale(scale, largest):
    return scale / jnp.sqrt(largest)


def partner(at, mask, size):
    out, bit = at, 1
    while bit < size:
        if mask & bit:
            out = out + bit * (1 - 2 * lax.rem(lax.div(at, bit), 2))
        bit *= 2
    return out


def kernel(
    n_prow, n_pcol, col_blocks, slots, width,
    brow_hbm, bcol_hbm, count_hbm, tiles_ref,
    row_out, col_out, brow_ref, bcol_ref, count_ref, meta_sem,
    block, row_split, col_vec, spread_a, spread_b, peak_a, peak_b,
    row_send, part_recv, done_send, done_recv, col_send, col_recv,
    load_sem, part_send_sem, part_recv_sem,
    done_send_sem, done_recv_sem, col_send_sem, col_recv_sem,
):
    def load(t):
        at = pl.ds(t * STEP, STEP)
        return pltpu.make_async_copy(tiles_ref.at[at], block.at[at], load_sem.at[t])

    for t in range(slots // STEP):
        load(t).start()
    metas = [
        pltpu.make_async_copy(brow_hbm, brow_ref, meta_sem.at[0]),
        pltpu.make_async_copy(bcol_hbm, bcol_ref, meta_sem.at[1]),
        pltpu.make_async_copy(count_hbm, count_ref, meta_sem.at[2]),
    ]
    for m in metas:
        m.start()

    pr = lax.axis_index("prow")
    pc = lax.axis_index("pcol")
    barrier = pltpu.get_barrier_semaphore()
    for d in range(1, n_pcol):
        pl.semaphore_signal(barrier, inc=1, device_id={"pcol": lax.rem(pc + d, n_pcol)})
    for d in range(1, n_prow):
        pl.semaphore_signal(barrier, inc=1, device_id={"prow": lax.rem(pr + d, n_prow)})

    for m in metas:
        m.wait()
    count = count_ref[0]
    row_ids = lax.broadcasted_iota(jnp.int32, (BR_DEV, width), 0)
    col_ids = lax.broadcasted_iota(jnp.int32, (col_blocks, width), 0)
    lane_ids = lax.broadcasted_iota(jnp.int32, (1, LANES), 1)
    ones = jnp.ones((LANES, LANES), jnp.bfloat16)
    lane_full = lax.broadcasted_iota(jnp.int32, (8, LANES), 1)
    lane_group = lane_full // 8
    own_lane = lane_full % 8 == lax.broadcasted_iota(jnp.int32, (8, LANES), 0)
    halves = width // LANES
    peak_b[...] = jnp.zeros_like(peak_b)

    def spread_rows(s, out, j):
        brow = brow_ref[jnp.minimum(s, slots - 1)]
        pick = jnp.where(
            (lane_ids % BR_DEV == brow) & (lane_ids < 3 * BR_DEV), 1.0, 0.0
        ).astype(jnp.bfloat16)
        out[j] = jnp.dot(row_split[...] * pick, ones, preferred_element_type=jnp.float32)

    def scale_tile(s, spread, peak, j, col_acc):
        bcol = bcol_ref[s]
        if spread is not None:
            cols = col_vec[pl.ds(bcol, 1), :]
        col_part = [None] * halves
        for g in range(width // ROWS):
            at = slice(g * ROWS, (g + 1) * ROWS)
            best = None
            for h in range(halves):
                lanes = slice(h * LANES, (h + 1) * LANES)
                x = jnp.abs(block[s, at, lanes]).astype(jnp.float32)
                if spread is not None:
                    x = (x * spread[j, at, :]) * cols[:, lanes]
                col_part[h] = x if g == 0 else jnp.maximum(col_part[h], x)
                best = x if h == 0 else jnp.maximum(best, x)
            peak[j, at, :] = best
        top = jnp.concatenate([jnp.max(c, axis=0, keepdims=True) for c in col_part], axis=1)
        col_at = jnp.where(s < count, bcol, -1)
        return jnp.maximum(col_acc, jnp.where(col_ids == col_at, top, 0.0))

    def reduce_rows(s, peak, j, row_acc):
        parts = []
        for h in range(halves):
            packed = None
            for g in range(LANES // 8):
                at = h * LANES + 8 * g
                best = jnp.max(peak[j, at:at + 8, :], axis=1, keepdims=True)
                best = jnp.broadcast_to(best, (8, LANES))
                packed = best if g == 0 else jnp.where(lane_group == g, best, packed)
            parts.append(jnp.max(jnp.where(own_lane, packed, 0.0), axis=0, keepdims=True))
        row_at = jnp.where((s >= 0) & (s < count), brow_ref[jnp.maximum(s, 0)], -1)
        return jnp.maximum(
            row_acc, jnp.where(row_ids == row_at, jnp.concatenate(parts, axis=1), 0.0)
        )

    def four_tiles(t, carry, first):
        row_acc, col_acc = carry
        base = t * STEP
        if first:
            load(t).wait()
        for part in range(2):
            here, peak = (spread_a, peak_a) if part == 0 else (spread_b, peak_b)
            there, last = (spread_b, peak_b) if part == 0 else (spread_a, peak_a)
            s = base + 2 * part
            if not first:
                for j in range(2):
                    spread_rows(s + 2 + j, there, j)
            for j in range(2):
                row_acc = reduce_rows(s - 2 + j, last, j, row_acc)
            for j in range(2):
                col_acc = scale_tile(s + j, None if first else here, peak, j, col_acc)
        return row_acc, col_acc

    row_vec = jnp.ones((BR_DEV, width), jnp.float32)
    col_now = jnp.ones((col_blocks, width), jnp.float32)
    share = BR_DEV // n_pcol
    for sweep in range(SWEEPS):
        if sweep > 0:
            for j in range(2):
                spread_rows(j, spread_a, j)
        row_max, col_max = lax.fori_loop(
            0, slots // STEP, functools.partial(four_tiles, first=sweep == 0),
            (jnp.zeros((BR_DEV, width), jnp.float32), jnp.zeros((col_blocks, width), jnp.float32)),
        )
        col_send[sweep] = col_max
        for j in range(2):
            row_max = reduce_rows(slots - 2 + j, peak_b, j, row_max)
        row_send[sweep] = row_max
        if sweep == 0:
            pl.semaphore_wait(barrier, n_pcol - 1 + n_prow - 1)
        part_copies = []
        for d in range(n_pcol - 1, 0, -1):
            to = partner(pc, d, n_pcol)
            part_copies.append(pltpu.make_async_remote_copy(
                src_ref=row_send.at[sweep], dst_ref=part_recv.at[sweep, d - 1],
                send_sem=part_send_sem.at[sweep, d - 1], recv_sem=part_recv_sem.at[sweep, d - 1],
                device_id={"pcol": to},
            ))
        for copy in part_copies:
            copy.start()
        col_copies = []
        for d in range(1, n_prow):
            col_copies.append(pltpu.make_async_remote_copy(
                src_ref=col_send.at[sweep], dst_ref=col_recv.at[sweep, d - 1],
                send_sem=col_send_sem.at[sweep, d - 1], recv_sem=col_recv_sem.at[sweep, d - 1],
                device_id={"prow": lax.rem(pr + d, n_prow)},
            ))
        for copy in col_copies:
            copy.start()
        for d, copy in enumerate(col_copies):
            copy.wait()
            col_max = jnp.maximum(col_max, col_recv[sweep, d])
        col_now = rescale(col_now, col_max)
        for d, copy in enumerate(part_copies):
            copy.wait()
            row_max = jnp.maximum(row_max, part_recv[sweep, n_pcol - 2 - d])
        row_vec = rescale(row_vec, row_max)
        if sweep + 1 < SWEEPS:
            col_vec[...] = col_now
            top = row_vec.astype(jnp.bfloat16).astype(jnp.float32)
            left = row_vec - top
            mid = left.astype(jnp.bfloat16).astype(jnp.float32)
            low = left - mid
            rest = jnp.zeros((LANES - 3 * BR_DEV, width), jnp.float32)
            stack = jnp.concatenate([top, mid, low, rest], axis=0)
            for h in range(halves):
                row_split[h * LANES:(h + 1) * LANES, :] = (
                    stack[:, h * LANES:(h + 1) * LANES].T.astype(jnp.bfloat16)
                )
    row_out[...] = row_vec
    col_out[...] = col_now


def spell(row_ref, col_ref, row_out, col_out):
    for ref, out in ((row_ref, row_out), (col_ref, col_out)):
        for i in range(ref.shape[0]):
            out[i] = ref[i:i + 1, :]


def solution(mesh):
    n_prow, n_pcol = mesh.shape["prow"], mesh.shape["pcol"]

    def on_device(tiles, tile_brow, tile_bcol, tile_count):
        slots, width = tiles.shape[2], tiles.shape[3]
        col_blocks = BR_DEV * n_prow // n_pcol
        share = BR_DEV // n_pcol
        anyb = pl.BlockSpec(memory_space=pl.ANY)
        vmem = pl.BlockSpec(memory_space=pltpu.VMEM)
        row_vec, col_vec = pl.pallas_call(
            functools.partial(kernel, n_prow, n_pcol, col_blocks, slots, width),
            out_shape=(
                jax.ShapeDtypeStruct((BR_DEV, width), jnp.float32),
                jax.ShapeDtypeStruct((col_blocks, width), jnp.float32),
            ),
            in_specs=[anyb, anyb, anyb, pl.BlockSpec(memory_space=pl.ANY)],
            out_specs=(vmem, vmem),
            scratch_shapes=[
                pltpu.SMEM((slots,), jnp.int32), pltpu.SMEM((slots,), jnp.int32), pltpu.SMEM((1,), jnp.int32), pltpu.SemaphoreType.DMA((3,)),
                pltpu.VMEM((slots, width, width), jnp.bfloat16),
                pltpu.VMEM((width, LANES), jnp.bfloat16),
                pltpu.VMEM((col_blocks, width), jnp.float32),
                pltpu.VMEM((2, width, LANES), jnp.float32),
                pltpu.VMEM((2, width, LANES), jnp.float32),
                pltpu.VMEM((2, width, LANES), jnp.float32),
                pltpu.VMEM((2, width, LANES), jnp.float32),
                pltpu.VMEM((SWEEPS, BR_DEV, width), jnp.float32),
                pltpu.VMEM((SWEEPS, n_pcol - 1, BR_DEV, width), jnp.float32),
                pltpu.VMEM((SWEEPS, share, width), jnp.float32),
                pltpu.VMEM((SWEEPS, n_pcol, share, width), jnp.float32),
                pltpu.VMEM((SWEEPS, col_blocks, width), jnp.float32),
                pltpu.VMEM((SWEEPS, n_prow - 1, col_blocks, width), jnp.float32),
                pltpu.SemaphoreType.DMA((slots // STEP,)),
                pltpu.SemaphoreType.DMA((SWEEPS, n_pcol - 1)),
                pltpu.SemaphoreType.DMA((SWEEPS, n_pcol - 1)),
                pltpu.SemaphoreType.DMA((SWEEPS, n_pcol - 1)),
                pltpu.SemaphoreType.DMA((SWEEPS, n_pcol - 1)),
                pltpu.SemaphoreType.DMA((SWEEPS, n_prow - 1)),
                pltpu.SemaphoreType.DMA((SWEEPS, n_prow - 1)),
            ],
            compiler_params=pltpu.CompilerParams(collective_id=0, has_side_effects=True, vmem_limit_bytes=53 << 20),
        )(
            pltpu.with_memory_space_constraint(tile_brow.reshape(slots), pltpu.HBM), pltpu.with_memory_space_constraint(tile_bcol.reshape(slots), pltpu.HBM), tile_count.reshape(1),
            tiles.reshape(slots, width, width),
        )
        return pl.pallas_call(
            spell,
            out_shape=(
                jax.ShapeDtypeStruct((BR_DEV, 1, width), jnp.float32),
                jax.ShapeDtypeStruct((col_blocks, 1, width), jnp.float32),
            ),
            in_specs=[vmem, vmem],
            out_specs=(vmem, vmem),
            compiler_params=pltpu.CompilerParams(vmem_limit_bytes=4 << 20),
        )(row_vec, col_vec)

    return jax.shard_map(
        on_device,
        mesh=mesh,
        in_specs=(
            P("prow", "pcol", None, None, None),
            P("prow", "pcol", None),
            P("prow", "pcol", None),
            P("prow", "pcol"),
        ),
        out_specs=(P(None, "prow", None), P(None, "pcol", None)),
        check_vma=False,
    )
```

```python
import functools
import math

import jax
import jax.numpy as jnp
from jax import lax
from jax.experimental import pallas as pl
from jax.experimental.pallas import tpu as pltpu
from jax.sharding import PartitionSpec as P

BR_DEV = 32
SWEEPS = 3
LANES = 128
SUB = 8
STEP = 4
PACK = 16
LIFT = 2.0 ** 63


def rescale(scale, largest):
    return scale / jnp.sqrt(largest)


def partner(at, mask, size):
    out, bit = at, 1
    while bit < size:
        if mask & bit:
            out = out + bit * (1 - 2 * lax.rem(lax.div(at, bit), 2))
        bit *= 2
    return out


def kernel(
    n_prow, n_pcol, col_blocks, slots, width,
    brow_hbm, bcol_hbm, count_hbm, tiles_ref,
    row_out, col_out,
    brow_ref, bcol_ref, count_ref,
    block, plain, turned, row_slot, col_slot, split, spread_a, spread_b, col_vec,
    ids, row_buf, col_buf,
    meta_sem, load_sem, ids_send_sem, ids_recv_sem,
    row_send_sem, row_recv_sem, col_send_sem, col_recv_sem,
):
    halves = width // LANES
    group = math.gcd(n_prow, n_pcol)
    few = slots // 2
    pr = lax.axis_index("prow")
    pc = lax.axis_index("pcol")
    holder = lax.rem(pc, group) == lax.rem(pr, group)
    steps = jnp.where(holder, slots, few) // STEP

    def load(t):
        at = pl.ds(t * STEP, STEP)
        return pltpu.make_async_copy(tiles_ref.at[at], block.at[at], load_sem.at[t])

    for t in range(few // STEP):
        load(t).start()

    @pl.when(holder)
    def _():
        for t in range(few // STEP, slots // STEP):
            load(t).start()

    metas = [
        pltpu.make_async_copy(brow_hbm, brow_ref, meta_sem.at[0]),
        pltpu.make_async_copy(bcol_hbm, bcol_ref, meta_sem.at[1]),
        pltpu.make_async_copy(count_hbm, count_ref, meta_sem.at[2]),
    ]
    for meta in metas:
        meta.start()
    barrier = pltpu.get_barrier_semaphore()
    for m in range(1, n_pcol):
        pl.semaphore_signal(barrier, inc=1, device_id={"pcol": partner(pc, m, n_pcol)})
    for m in range(1, n_prow):
        pl.semaphore_signal(barrier, inc=1, device_id={"prow": partner(pr, m, n_prow)})

    row_ids = lax.broadcasted_iota(jnp.int32, (BR_DEV, LANES), 0)
    col_ids = lax.broadcasted_iota(jnp.int32, (col_blocks, LANES), 0)
    pick_row = lax.broadcasted_iota(jnp.int32, (LANES, 2 * LANES), 0)
    pick_lane = lax.broadcasted_iota(jnp.int32, (1, 2 * LANES), 1)

    def lanes(h):
        return slice(h * LANES, (h + 1) * LANES)

    def widest(parts):
        while len(parts) > 1:
            pairs = [jnp.maximum(a, b) for a, b in zip(parts[::2], parts[1::2])]
            parts = pairs + parts[len(parts) - len(parts) % 2:]
        return parts[0]

    def keep(ref, s, h, top):
        ref[h, pl.ds(pl.multiple_of(s * SUB, SUB), SUB), :] = top

    def tops(ref, h, n):
        return widest([ref[h, pl.ds(k, n, stride=SUB), :] for k in range(SUB)])

    def first_tile(s):
        x = [[jnp.abs(block[s, g * PACK:(g + 1) * PACK, lanes(h)]) for h in range(halves)]
             for g in range(width // PACK)]
        for h in range(halves):
            top = widest([row[h] for row in x]).astype(jnp.float32)
            keep(col_slot, s, h, jnp.maximum(top[:SUB], top[SUB:]))
        fold = jnp.concatenate([widest(row) for row in x], axis=0).T
        top = widest([fold[k * PACK:(k + 1) * PACK] for k in range(LANES // PACK)])
        top = top.astype(jnp.float32)
        top = jnp.maximum(top[:SUB], top[SUB:])
        for h in range(halves):
            keep(row_slot, s, h, top[:, lanes(h)])

    def first_step(t, carry):
        load(t).wait()
        for j in range(STEP):
            first_tile(t * STEP + j)
        return carry

    def prepare(s, carry):
        x = jnp.abs(block[s])
        plain[s] = x.astype(jnp.float32)
        turned[s] = x.T.astype(jnp.float32)
        return carry

    def set_split(vec):
        n = vec.shape[0]
        top = vec.astype(jnp.bfloat16)
        left = vec - top.astype(jnp.float32)
        mid = left.astype(jnp.bfloat16)
        low = (left - mid.astype(jnp.float32)).astype(jnp.bfloat16)
        rest = jnp.zeros((LANES - 3 * n, width), jnp.bfloat16)
        stack = jnp.concatenate([top, mid, low, rest], axis=0)
        for h in range(halves):
            split[lanes(h), :] = stack[:, lanes(h)].T

    def spread_pair(ids_ref, n, s, out):
        a = ids_ref[jnp.minimum(s, slots - 1)]
        b = ids_ref[jnp.minimum(s + 1, slots - 1)]
        want = jnp.where(pick_lane < LANES, a, b)
        hit = (pick_row == want) | (pick_row == want + n) | (pick_row == want + 2 * n)
        pick = jnp.where(hit, 1.0, 0.0).astype(jnp.bfloat16)
        out[...] = jnp.dot(split[...], pick, preferred_element_type=jnp.float32)

    def scale_tile(data, s, j, spread, slot, store):
        best = [[None, None] for _ in range(halves)]
        for g in range(width // SUB):
            at = slice(g * SUB, (g + 1) * SUB)
            by = spread[at, lanes(j)]
            for h in range(halves):
                x = data[s, at, lanes(h)] * by
                if store:
                    data[s, at, lanes(h)] = x
                old = best[h][g % 2]
                best[h][g % 2] = x if old is None else jnp.maximum(old, x)
        for h in range(halves):
            keep(slot, s, h, jnp.maximum(*best[h]))

    def one_pass(data, vec, ids_ref, slot, store):
        set_split(vec)
        n = vec.shape[0]
        spread_pair(ids_ref, n, 0, spread_a)

        def body(t, carry):
            s = t * STEP
            spread_pair(ids_ref, n, s + 2, spread_b)
            for j in range(2):
                scale_tile(data, s + j, j, spread_a, slot, store)
            spread_pair(ids_ref, n, s + 4, spread_a)
            for j in range(2):
                scale_tile(data, s + 2 + j, j, spread_b, slot, store)
            return carry

        lax.fori_loop(0, steps, body, 0)

    def live_id(ref, s):
        return jnp.where(s < count_ref[0], ref[s], -1)

    def gather_slots(ref, ids_ref, where_ids, n, out):
        for h in range(halves):
            top = tops(ref, h, n)
            acc = jnp.zeros(where_ids.shape, jnp.float32)
            for s in range(n):
                acc = jnp.maximum(
                    acc, jnp.where(where_ids == live_id(ids_ref, s), top[s:s + 1, :], 0.0)
                )
            out[:, lanes(h)] = acc

    def row_copies(k, rows):
        return [pltpu.make_async_remote_copy(
            src_ref=row_buf.at[k, pc, pl.ds(0, rows)], dst_ref=row_buf.at[k, pc, pl.ds(0, rows)],
            send_sem=row_send_sem.at[k, m - 1], recv_sem=row_recv_sem.at[k, pc],
            device_id={"pcol": partner(pc, m, n_pcol)},
        ) for m in range(n_pcol - 1, 0, -1)]

    def ids_copies():
        return [pltpu.make_async_remote_copy(
            src_ref=ids.at[pc], dst_ref=ids.at[pc],
            send_sem=ids_send_sem.at[m - 1], recv_sem=ids_recv_sem.at[pc],
            device_id={"pcol": partner(pc, m, n_pcol)},
        ) for m in range(n_pcol - 1, 0, -1)]

    def col_copies(k):
        return [pltpu.make_async_remote_copy(
            src_ref=col_buf.at[k, pr], dst_ref=col_buf.at[k, pr],
            send_sem=col_send_sem.at[k, m - 1], recv_sem=col_recv_sem.at[k, pr],
            device_id={"prow": partner(pr, m, n_prow)},
        ) for m in range(n_prow - 1, 0, -1)]

    def send_rows(k):
        @pl.when(holder)
        def _():
            gather_slots(row_slot, brow_ref, row_ids, slots, row_buf.at[k, pc])
            for copy in row_copies(k, BR_DEV):
                copy.start()

        @pl.when(jnp.logical_not(holder))
        def _():
            for h in range(halves):
                row_buf[k, pc, :few, lanes(h)] = tops(row_slot, h, few)
            for copy in row_copies(k, few):
                copy.start()

    def send_cols(k):
        @pl.when(holder)
        def _():
            gather_slots(col_slot, bcol_ref, col_ids, slots, col_buf.at[k, pr])

        @pl.when(jnp.logical_not(holder))
        def _():
            gather_slots(col_slot, bcol_ref, col_ids, few, col_buf.at[k, pr])

        for copy in col_copies(k):
            copy.start()

    def arrived(copy):
        copy.wait_recv()

    def wait_rows(k):
        per = n_pcol // group

        def from_few(i, acc):
            q = lax.rem(lax.rem(pr, group) + 1 + lax.div(i, per), group) + group * lax.rem(i, per)

            @pl.when(q != pc)
            def _():
                ref = row_buf.at[k, q, pl.ds(0, few)]
                pltpu.make_async_remote_copy(
                    src_ref=ref, dst_ref=ref, send_sem=row_send_sem.at[k, 0],
                    recv_sem=row_recv_sem.at[k, q], device_id={"pcol": q},
                ).wait_recv()
                if k == 0:
                    pltpu.make_async_remote_copy(
                        src_ref=ids.at[q], dst_ref=ids.at[q], send_sem=ids_send_sem.at[0],
                        recv_sem=ids_recv_sem.at[q], device_id={"pcol": q},
                    ).wait_recv()

            acc = list(acc)
            for s in range(few):
                hit = row_ids == ids[q, s:s + 1, :]
                for h in range(halves):
                    top = row_buf[k, q, s:s + 1, lanes(h)]
                    acc[h] = jnp.maximum(acc[h], jnp.where(hit, top, 0.0))
            return tuple(acc)

        acc = lax.fori_loop(
            0, n_pcol - per, from_few,
            tuple(jnp.zeros((BR_DEV, LANES), jnp.float32) for _ in range(halves)),
        )
        acc = jnp.concatenate(acc, axis=1)
        for i in range(per):
            q = lax.rem(pr, group) + group * i

            @pl.when(q != pc)
            def _():
                ref = row_buf.at[k, q]
                pltpu.make_async_remote_copy(
                    src_ref=ref, dst_ref=ref, send_sem=row_send_sem.at[k, 0],
                    recv_sem=row_recv_sem.at[k, q], device_id={"pcol": q},
                ).wait_recv()

            acc = jnp.maximum(acc, row_buf[k, q])
        return acc

    def wait_cols(k):
        for m in range(n_prow - 1, 0, -1):
            q = partner(pr, m, n_prow)
            ref = col_buf.at[k, q]
            pltpu.make_async_remote_copy(
                src_ref=ref, dst_ref=ref, send_sem=col_send_sem.at[k, m - 1],
                recv_sem=col_recv_sem.at[k, q], device_id={"prow": q},
            ).wait_recv()
        return widest([col_buf[k, q] for q in range(n_prow)])

    lax.fori_loop(0, steps, first_step, 0)
    for meta in metas:
        meta.wait()
    pl.semaphore_wait(barrier, n_pcol - 1 + n_prow - 1)
    send_rows(0)
    send_cols(0)

    @pl.when(jnp.logical_not(holder))
    def _():
        for s in range(few):
            ids[pc, s:s + 1, :] = jnp.full((1, LANES), live_id(brow_ref, s), jnp.int32)
        for copy in ids_copies():
            copy.start()

    lax.fori_loop(0, steps * STEP, prepare, 0)

    one = jnp.ones((BR_DEV, width), jnp.float32)
    row_1 = rescale(one, wait_rows(0))
    one_pass(plain, row_1, brow_ref, col_slot, False)
    send_cols(1)
    col_1 = rescale(jnp.ones((col_blocks, width), jnp.float32), wait_cols(0))
    lifted = col_1 * LIFT
    one_pass(turned, lifted, bcol_ref, row_slot, True)
    send_rows(1)
    col_vec[...] = lifted

    def lift_plain(s, carry):
        by = col_vec[pl.ds(bcol_ref[s], 1), :]
        plain[s] = plain[s] * by
        return carry

    lax.fori_loop(0, steps * STEP, lift_plain, 0)
    col_max = col_1 * wait_cols(1)
    col_2 = rescale(col_1, col_max)
    change = 1.0 / jnp.sqrt(col_max)
    one_pass(turned, change, bcol_ref, row_slot, False)
    send_rows(2)
    row_2 = rescale(row_1, (row_1 * wait_rows(1)) / LIFT)
    one_pass(plain, row_2, brow_ref, col_slot, False)
    send_cols(2)
    row_out[...] = rescale(row_2, (row_2 * wait_rows(2)) / LIFT)
    col_out[...] = rescale(col_2, (change * wait_cols(2)) / LIFT)

    for k in range(SWEEPS):
        @pl.when(holder)
        def _():
            for copy in row_copies(k, BR_DEV):
                copy.wait_send()

        @pl.when(jnp.logical_not(holder))
        def _():
            for copy in row_copies(k, few):
                copy.wait_send()
            if k == 0:
                for copy in ids_copies():
                    copy.wait_send()

        for copy in col_copies(k):
            copy.wait_send()


def spell(row_ref, col_ref, row_out, col_out):
    for ref, out in ((row_ref, row_out), (col_ref, col_out)):
        for i in range(ref.shape[0]):
            out[i] = ref[i:i + 1, :]


def solution(mesh):
    n_prow, n_pcol = mesh.shape["prow"], mesh.shape["pcol"]

    def on_device(tiles, tile_brow, tile_bcol, tile_count):
        slots, width = tiles.shape[2], tiles.shape[3]
        col_blocks = BR_DEV * n_prow // n_pcol
        halves = width // LANES
        vmem = pl.BlockSpec(memory_space=pltpu.VMEM)
        anywhere = pl.BlockSpec(memory_space=pl.ANY)
        row_vec, col_vec = pl.pallas_call(
            functools.partial(kernel, n_prow, n_pcol, col_blocks, slots, width),
            out_shape=(
                jax.ShapeDtypeStruct((BR_DEV, width), jnp.float32),
                jax.ShapeDtypeStruct((col_blocks, width), jnp.float32),
            ),
            in_specs=[anywhere] * 4,
            out_specs=(vmem, vmem),
            scratch_shapes=[
                pltpu.SMEM((slots,), jnp.int32),
                pltpu.SMEM((slots,), jnp.int32),
                pltpu.SMEM((1,), jnp.int32),
                pltpu.VMEM((slots, width, width), jnp.bfloat16),
                pltpu.VMEM((slots, width, width), jnp.float32),
                pltpu.VMEM((slots, width, width), jnp.float32),
                pltpu.VMEM((halves, slots * SUB, LANES), jnp.float32),
                pltpu.VMEM((halves, slots * SUB, LANES), jnp.float32),
                pltpu.VMEM((width, LANES), jnp.bfloat16),
                pltpu.VMEM((width, 2 * LANES), jnp.float32),
                pltpu.VMEM((width, 2 * LANES), jnp.float32),
                pltpu.VMEM((col_blocks, width), jnp.float32),
                pltpu.VMEM((n_pcol, slots // 2, LANES), jnp.int32),
                pltpu.VMEM((SWEEPS, n_pcol, BR_DEV, width), jnp.float32),
                pltpu.VMEM((SWEEPS, n_prow, col_blocks, width), jnp.float32),
                pltpu.SemaphoreType.DMA((3,)),
                pltpu.SemaphoreType.DMA((slots // STEP,)),
                pltpu.SemaphoreType.DMA((n_pcol - 1,)),
                pltpu.SemaphoreType.DMA((n_pcol,)),
                pltpu.SemaphoreType.DMA((SWEEPS, n_pcol - 1)),
                pltpu.SemaphoreType.DMA((SWEEPS, n_pcol)),
                pltpu.SemaphoreType.DMA((SWEEPS, n_prow - 1)),
                pltpu.SemaphoreType.DMA((SWEEPS, n_prow)),
            ],
            compiler_params=pltpu.CompilerParams(
                collective_id=0, has_side_effects=True, vmem_limit_bytes=53 << 20
            ),
        )(
            pltpu.with_memory_space_constraint(tile_brow.reshape(slots), pltpu.HBM),
            pltpu.with_memory_space_constraint(tile_bcol.reshape(slots), pltpu.HBM),
            tile_count.reshape(1),
            tiles.reshape(slots, width, width),
        )
        return pl.pallas_call(
            spell,
            out_shape=(
                jax.ShapeDtypeStruct((BR_DEV, 1, width), jnp.float32),
                jax.ShapeDtypeStruct((col_blocks, 1, width), jnp.float32),
            ),
            in_specs=[vmem, vmem],
            out_specs=(vmem, vmem),
            compiler_params=pltpu.CompilerParams(vmem_limit_bytes=4 << 20),
        )(row_vec, col_vec)

    return jax.shard_map(
        on_device,
        mesh=mesh,
        in_specs=(
            P("prow", "pcol", None, None, None),
            P("prow", "pcol", None),
            P("prow", "pcol", None),
            P("prow", "pcol"),
        ),
        out_specs=(P(None, "prow", None), P(None, "pcol", None)),
        check_vma=False,
    )
```

```python
import functools
import math

import jax
import jax.numpy as jnp
from jax import lax
from jax.experimental import pallas as pl
from jax.experimental.pallas import tpu as pltpu
from jax.sharding import PartitionSpec as P

BR_DEV = 32
SWEEPS = 3
LANES = 128
SUB = 8
STEP = 4
PACK = 16
LIFT = 2.0 ** 63


def rescale(scale, largest):
    return scale / jnp.sqrt(largest)


def partner(at, mask, size):
    out, bit = at, 1
    while bit < size:
        if mask & bit:
            out = out + bit * (1 - 2 * lax.rem(lax.div(at, bit), 2))
        bit *= 2
    return out


def kernel(
    n_prow, n_pcol, col_blocks, slots, width,
    brow_hbm, bcol_hbm, count_hbm, tiles_ref,
    row_out, col_out,
    brow_ref, bcol_ref, count_ref,
    block, plain, turned, row_slot, col_slot, split, spread, row_table, col_table, row_vec, slot_top, own_ids,
    ids, row_buf, col_buf,
    meta_sem, load_sem, ids_send_sem, ids_recv_sem,
    row_send_sem, row_recv_sem, col_send_sem, col_recv_sem,
):
    halves = width // LANES
    group = math.gcd(n_prow, n_pcol)
    few = slots // 2
    pr = lax.axis_index("prow")
    pc = lax.axis_index("pcol")
    holder = lax.rem(pc, group) == lax.rem(pr, group)
    steps = jnp.where(holder, slots, few) // STEP

    def load(t):
        at = pl.ds(t * STEP, STEP)
        return pltpu.make_async_copy(tiles_ref.at[at], block.at[at], load_sem.at[t])

    for t in range(few // STEP):
        load(t).start()

    @pl.when(holder)
    def _():
        for t in range(few // STEP, slots // STEP):
            load(t).start()

    metas = [
        pltpu.make_async_copy(brow_hbm, brow_ref, meta_sem.at[0]),
        pltpu.make_async_copy(bcol_hbm, bcol_ref, meta_sem.at[1]),
        pltpu.make_async_copy(count_hbm, count_ref, meta_sem.at[2]),
    ]
    for meta in metas:
        meta.start()
    barrier = pltpu.get_barrier_semaphore()
    for m in range(1, n_pcol):
        pl.semaphore_signal(barrier, inc=1, device_id={"pcol": partner(pc, m, n_pcol)})
    for m in range(1, n_prow):
        pl.semaphore_signal(barrier, inc=1, device_id={"prow": partner(pr, m, n_prow)})

    row_ids = lax.broadcasted_iota(jnp.int32, (BR_DEV, LANES), 0)
    col_ids = lax.broadcasted_iota(jnp.int32, (col_blocks, LANES), 0)
    line = lax.broadcasted_iota(jnp.int32, (LANES, LANES), 0)
    for table, n in ((row_table, BR_DEV), (col_table, col_blocks)):
        turn = jnp.where(line < 3 * n, lax.rem(line, n), -2)
        turn = turn.astype(jnp.float32).astype(jnp.bfloat16)
        for i in range(n):
            table[i] = jnp.maximum(1.0 - jnp.abs(turn - float(i)), 0.0).astype(jnp.bfloat16)

    def lanes(h):
        return slice(h * LANES, (h + 1) * LANES)

    def widest(parts):
        while len(parts) > 1:
            pairs = [jnp.maximum(a, b) for a, b in zip(parts[::2], parts[1::2])]
            parts = pairs + parts[len(parts) - len(parts) % 2:]
        return parts[0]

    def keep(ref, s, h, top):
        ref[h, pl.ds(pl.multiple_of(s * SUB, SUB), SUB), :] = top

    def tops(ref, h, n):
        return widest([ref[h, pl.ds(k, n, stride=SUB), :] for k in range(SUB)])

    def first_tile(s):
        x = [[jnp.abs(block[s, g * PACK:(g + 1) * PACK, lanes(h)]) for h in range(halves)]
             for g in range(width // PACK)]
        for h in range(halves):
            top = widest([row[h] for row in x]).astype(jnp.float32)
            keep(col_slot, s, h, jnp.maximum(top[:SUB], top[SUB:]))
        fold = jnp.concatenate([widest(row) for row in x], axis=0).T
        top = widest([fold[k * PACK:(k + 1) * PACK] for k in range(LANES // PACK)])
        top = top.astype(jnp.float32)
        top = jnp.maximum(top[:SUB], top[SUB:])
        for h in range(halves):
            keep(row_slot, s, h, top[:, lanes(h)])

    def first_step(t, carry):
        load(t).wait()
        for j in range(STEP):
            first_tile(t * STEP + j)
        return carry

    def prepare(s, carry):
        x = jnp.abs(block[s])
        plain[s] = x.astype(jnp.float32)
        turned[s] = x.T.astype(jnp.float32)
        return carry

    def set_split(vec):
        n = vec.shape[0]
        top = vec.astype(jnp.bfloat16)
        left = vec - top.astype(jnp.float32)
        mid = left.astype(jnp.bfloat16)
        low = (left - mid.astype(jnp.float32)).astype(jnp.bfloat16)
        rest = jnp.zeros((LANES - 3 * n, width), jnp.bfloat16)
        stack = jnp.concatenate([top, mid, low, rest], axis=0)
        for h in range(halves):
            split[lanes(h), :] = stack[:, lanes(h)].T

    def spread_pair(ids_ref, table, p):
        pick = jnp.concatenate([table[ids_ref[2 * p + j]] for j in range(2)], axis=1)
        spread[p] = jnp.dot(split[...], pick, preferred_element_type=jnp.float32)

    def scale_tile(data, s, slot):
        best = [[None, None] for _ in range(halves)]
        for g in range(width // SUB):
            at = slice(g * SUB, (g + 1) * SUB)
            by = spread[s // 2, at, lanes(s % 2)]
            for h in range(halves):
                x = data[s, at, lanes(h)] * by
                old = best[h][g % 2]
                best[h][g % 2] = x if old is None else jnp.maximum(old, x)
        for h in range(halves):
            keep(slot, s, h, jnp.maximum(*best[h]))

    def one_pass(data, vec, ids_ref, slot):
        set_split(vec)
        table = row_table if ids_ref is brow_ref else col_table
        half, pairs = few // 2, slots // 2
        ahead = half + half // 2
        for p in range(ahead):
            spread_pair(ids_ref, table, p)
            if 2 <= p < half + 2:
                for j in range(2):
                    scale_tile(data, 2 * (p - 2) + j, slot)

        @pl.when(holder)
        def _():
            for p in range(ahead, pairs):
                spread_pair(ids_ref, table, p)
            for s in range(few, slots):
                scale_tile(data, s, slot)

    def gather_slots(ref, kind, where_ids, n, out):
        for h in range(halves):
            slot_top[:n, lanes(h)] = tops(ref, h, n)
        acc = [jnp.zeros(where_ids.shape, jnp.float32) for _ in range(halves)]
        for s in range(n):
            hit = where_ids == own_ids[kind, s:s + 1, :]
            for h in range(halves):
                top = slot_top[s:s + 1, lanes(h)]
                acc[h] = jnp.maximum(acc[h], jnp.where(hit, top, 0.0))
        for h in range(halves):
            out[:, lanes(h)] = acc[h]

    def row_copies(k, rows):
        return [pltpu.make_async_remote_copy(
            src_ref=row_buf.at[k, pc, pl.ds(0, rows)], dst_ref=row_buf.at[k, pc, pl.ds(0, rows)],
            send_sem=row_send_sem.at[k, m - 1], recv_sem=row_recv_sem.at[k, pc],
            device_id={"pcol": partner(pc, m, n_pcol)},
        ) for m in range(n_pcol - 1, 0, -1)]

    def ids_copies():
        return [pltpu.make_async_remote_copy(
            src_ref=ids.at[pc], dst_ref=ids.at[pc],
            send_sem=ids_send_sem.at[m - 1], recv_sem=ids_recv_sem.at[pc],
            device_id={"pcol": partner(pc, m, n_pcol)},
        ) for m in range(n_pcol - 1, 0, -1)]

    def col_copies(k):
        return [pltpu.make_async_remote_copy(
            src_ref=col_buf.at[k, pr], dst_ref=col_buf.at[k, pr],
            send_sem=col_send_sem.at[k, m - 1], recv_sem=col_recv_sem.at[k, pr],
            device_id={"prow": partner(pr, m, n_prow)},
        ) for m in range(n_prow - 1, 0, -1)]

    def send_rows(k):
        @pl.when(holder)
        def _():
            gather_slots(row_slot, 1, row_ids, slots, row_buf.at[k, pc])
            for copy in row_copies(k, BR_DEV):
                copy.start()

        @pl.when(jnp.logical_not(holder))
        def _():
            for h in range(halves):
                row_buf[k, pc, :few, lanes(h)] = tops(row_slot, h, few)
            for copy in row_copies(k, few):
                copy.start()

    def send_cols(k):
        @pl.when(holder)
        def _():
            gather_slots(col_slot, 0, col_ids, slots, col_buf.at[k, pr])

        @pl.when(jnp.logical_not(holder))
        def _():
            gather_slots(col_slot, 0, col_ids, few, col_buf.at[k, pr])

        for copy in col_copies(k):
            copy.start()

    def arrived(copy):
        copy.wait_recv()

    def wait_rows(k):
        per = n_pcol // group

        def place(i):
            return lax.rem(lax.rem(pr, group) + 1 + lax.div(i, per), group) + group * lax.rem(i, per)

        def wait_few(i):
            q = place(i)

            @pl.when(q != pc)
            def _():
                ref = row_buf.at[k, q, pl.ds(0, few)]
                pltpu.make_async_remote_copy(
                    src_ref=ref, dst_ref=ref, send_sem=row_send_sem.at[k, 0],
                    recv_sem=row_recv_sem.at[k, q], device_id={"pcol": q},
                ).wait_recv()
                if k == 0:
                    pltpu.make_async_remote_copy(
                        src_ref=ids.at[q], dst_ref=ids.at[q], send_sem=ids_send_sem.at[0],
                        recv_sem=ids_recv_sem.at[q], device_id={"pcol": q},
                    ).wait_recv()

        def from_few(first, n, acc):
            for i in range(n):
                wait_few(first + i)
            acc = list(acc)
            for i in range(n):
                q = place(first + i)
                for s in range(few):
                    hit = row_ids == ids[q, s:s + 1, :]
                    for h in range(halves):
                        top = row_buf[k, q, s:s + 1, lanes(h)]
                        acc[h] = jnp.maximum(acc[h], jnp.where(hit, top, 0.0))
            return tuple(acc)

        zero = tuple(jnp.zeros((BR_DEV, LANES), jnp.float32) for _ in range(halves))
        rest, span = n_pcol - per, 3
        acc = lax.fori_loop(
            0, rest // span, lambda i, acc: from_few(i * span, span, acc), zero
        ) if rest > 2 * span else from_few(0, rest, zero)
        acc = jnp.concatenate(acc, axis=1)
        for i in range(per):
            q = lax.rem(pr, group) + group * i

            @pl.when(q != pc)
            def _():
                ref = row_buf.at[k, q]
                pltpu.make_async_remote_copy(
                    src_ref=ref, dst_ref=ref, send_sem=row_send_sem.at[k, 0],
                    recv_sem=row_recv_sem.at[k, q], device_id={"pcol": q},
                ).wait_recv()

            acc = jnp.maximum(acc, row_buf[k, q])
        return acc

    def wait_cols(k):
        for m in range(n_prow - 1, 0, -1):
            q = partner(pr, m, n_prow)
            ref = col_buf.at[k, q]
            pltpu.make_async_remote_copy(
                src_ref=ref, dst_ref=ref, send_sem=col_send_sem.at[k, m - 1],
                recv_sem=col_recv_sem.at[k, q], device_id={"prow": q},
            ).wait_recv()
        return widest([col_buf[k, q] for q in range(n_prow)])

    for meta in metas:
        meta.wait()
    for kind, ref in enumerate((bcol_ref, brow_ref)):
        for s in range(slots):
            own = jnp.where(s < count_ref[0], ref[s], -1)
            own_ids[kind, s:s + 1, :] = jnp.full((1, LANES), own, jnp.int32)
    ids[pc] = own_ids[1, :few]
    lax.fori_loop(0, steps, first_step, 0)
    pl.semaphore_wait(barrier, n_pcol - 1 + n_prow - 1)
    send_rows(0)
    send_cols(0)

    @pl.when(jnp.logical_not(holder))
    def _():
        for copy in ids_copies():
            copy.start()

    lax.fori_loop(0, steps * STEP, prepare, 0)

    one = jnp.ones((BR_DEV, width), jnp.float32)
    row_1 = rescale(one, wait_rows(0))
    one_pass(plain, row_1, brow_ref, col_slot)
    send_cols(1)
    col_1 = rescale(jnp.ones((col_blocks, width), jnp.float32), wait_cols(0))
    one_pass(turned, col_1 * LIFT, bcol_ref, row_slot)
    send_rows(1)
    row_vec[...] = row_1

    def scale_turned(s, carry):
        turned[s] = turned[s] * row_vec[pl.ds(brow_ref[s], 1), :]
        return carry

    lax.fori_loop(0, steps * STEP, scale_turned, 0)
    col_2 = rescale(col_1, col_1 * wait_cols(1))
    one_pass(turned, col_2, bcol_ref, row_slot)
    send_rows(2)
    row_max = (row_1 * wait_rows(1)) / LIFT
    row_2 = rescale(row_1, row_max)
    one_pass(plain, row_2, brow_ref, col_slot)
    send_cols(2)
    change = 1.0 / jnp.sqrt(row_max)
    row_out[...] = rescale(row_2, change * wait_rows(2))
    col_out[...] = rescale(col_2, col_2 * wait_cols(2))

    for k in range(SWEEPS):
        @pl.when(holder)
        def _():
            for copy in row_copies(k, BR_DEV):
                copy.wait_send()

        @pl.when(jnp.logical_not(holder))
        def _():
            for copy in row_copies(k, few):
                copy.wait_send()
            if k == 0:
                for copy in ids_copies():
                    copy.wait_send()

        for copy in col_copies(k):
            copy.wait_send()


def spell(row_ref, col_ref, row_out, col_out):
    for ref, out in ((row_ref, row_out), (col_ref, col_out)):
        for i in range(ref.shape[0]):
            out[i] = ref[i:i + 1, :]


def solution(mesh):
    n_prow, n_pcol = mesh.shape["prow"], mesh.shape["pcol"]

    def on_device(tiles, tile_brow, tile_bcol, tile_count):
        slots, width = tiles.shape[2], tiles.shape[3]
        col_blocks = BR_DEV * n_prow // n_pcol
        halves = width // LANES
        vmem = pl.BlockSpec(memory_space=pltpu.VMEM)
        anywhere = pl.BlockSpec(memory_space=pl.ANY)
        row_vec, col_vec = pl.pallas_call(
            functools.partial(kernel, n_prow, n_pcol, col_blocks, slots, width),
            out_shape=(
                jax.ShapeDtypeStruct((BR_DEV, width), jnp.float32),
                jax.ShapeDtypeStruct((col_blocks, width), jnp.float32),
            ),
            in_specs=[anywhere] * 4,
            out_specs=(vmem, vmem),
            scratch_shapes=[
                pltpu.SMEM((slots,), jnp.int32),
                pltpu.SMEM((slots,), jnp.int32),
                pltpu.SMEM((1,), jnp.int32),
                pltpu.VMEM((slots, width, width), jnp.bfloat16),
                pltpu.VMEM((slots, width, width), jnp.float32),
                pltpu.VMEM((slots, width, width), jnp.float32),
                pltpu.VMEM((halves, slots * SUB, LANES), jnp.float32),
                pltpu.VMEM((halves, slots * SUB, LANES), jnp.float32),
                pltpu.VMEM((width, LANES), jnp.bfloat16),
                pltpu.VMEM((slots // 2, width, 2 * LANES), jnp.float32),
                pltpu.VMEM((BR_DEV, LANES, LANES), jnp.bfloat16),
                pltpu.VMEM((col_blocks, LANES, LANES), jnp.bfloat16),
                pltpu.VMEM((BR_DEV, width), jnp.float32),
                pltpu.VMEM((slots, width), jnp.float32),
                pltpu.VMEM((2, slots, LANES), jnp.int32),
                pltpu.VMEM((n_pcol, slots // 2, LANES), jnp.int32),
                pltpu.VMEM((SWEEPS, n_pcol, BR_DEV, width), jnp.float32),
                pltpu.VMEM((SWEEPS, n_prow, col_blocks, width), jnp.float32),
                pltpu.SemaphoreType.DMA((3,)),
                pltpu.SemaphoreType.DMA((slots // STEP,)),
                pltpu.SemaphoreType.DMA((n_pcol - 1,)),
                pltpu.SemaphoreType.DMA((n_pcol,)),
                pltpu.SemaphoreType.DMA((SWEEPS, n_pcol - 1)),
                pltpu.SemaphoreType.DMA((SWEEPS, n_pcol)),
                pltpu.SemaphoreType.DMA((SWEEPS, n_prow - 1)),
                pltpu.SemaphoreType.DMA((SWEEPS, n_prow)),
            ],
            compiler_params=pltpu.CompilerParams(
                collective_id=0, has_side_effects=True, vmem_limit_bytes=53 << 20
            ),
        )(
            pltpu.with_memory_space_constraint(tile_brow.reshape(slots), pltpu.HBM),
            pltpu.with_memory_space_constraint(tile_bcol.reshape(slots), pltpu.HBM),
            tile_count.reshape(1),
            tiles.reshape(slots, width, width),
        )
        return pl.pallas_call(
            spell,
            out_shape=(
                jax.ShapeDtypeStruct((BR_DEV, 1, width), jnp.float32),
                jax.ShapeDtypeStruct((col_blocks, 1, width), jnp.float32),
            ),
            in_specs=[vmem, vmem],
            out_specs=(vmem, vmem),
            compiler_params=pltpu.CompilerParams(vmem_limit_bytes=4 << 20),
        )(row_vec, col_vec)

    return jax.shard_map(
        on_device,
        mesh=mesh,
        in_specs=(
            P("prow", "pcol", None, None, None),
            P("prow", "pcol", None),
            P("prow", "pcol", None),
            P("prow", "pcol"),
        ),
        out_specs=(P(None, "prow", None), P(None, "pcol", None)),
        check_vma=False,
    )
```

```python
import functools
import math

import jax
import jax.numpy as jnp
from jax import lax
from jax.experimental import pallas as pl
from jax.experimental.pallas import tpu as pltpu
from jax.sharding import PartitionSpec as P

BR_DEV = 32
SWEEPS = 3
LANES = 128
SUB = 8
STEP = 4
PACK = 16
LEAD = 2
LIFT = 2.0 ** 63


def rescale(scale, largest):
    return scale / jnp.sqrt(largest)


def partner(at, mask, size):
    out, bit = at, 1
    while bit < size:
        if mask & bit:
            out = out + bit * (1 - 2 * lax.rem(lax.div(at, bit), 2))
        bit *= 2
    return out


def kernel(
    n_prow, n_pcol, col_blocks, slots, width,
    brow_hbm, bcol_hbm, count_hbm, tiles_ref,
    row_out, col_out,
    brow_ref, bcol_ref, count_ref,
    block, plain, turned, row_slot, col_slot, split, spread, row_table, col_table, row_vec, slot_top, own_ids,
    ids_row, ids, row_buf, col_buf,
    meta_sem, load_sem, ids_send_sem, ids_recv_sem,
    row_send_sem, row_recv_sem, col_send_sem, col_recv_sem,
):
    halves = width // LANES
    group = math.gcd(n_prow, n_pcol)
    few = slots // 2
    pr = lax.axis_index("prow")
    pc = lax.axis_index("pcol")
    holder = lax.rem(pc, group) == lax.rem(pr, group)
    steps = jnp.where(holder, slots, few) // STEP

    def load(t):
        at = pl.ds(t * STEP, STEP)
        return pltpu.make_async_copy(tiles_ref.at[at], block.at[at], load_sem.at[t])

    for t in range(few // STEP):
        load(t).start()

    @pl.when(holder)
    def _():
        for t in range(few // STEP, slots // STEP):
            load(t).start()

    metas = [
        pltpu.make_async_copy(brow_hbm, brow_ref, meta_sem.at[0]),
        pltpu.make_async_copy(bcol_hbm, bcol_ref, meta_sem.at[1]),
        pltpu.make_async_copy(count_hbm, count_ref, meta_sem.at[2]),
    ]
    for meta in metas:
        meta.start()
    barrier = pltpu.get_barrier_semaphore()
    for m in range(1, n_pcol):
        pl.semaphore_signal(barrier, inc=1, device_id={"pcol": partner(pc, m, n_pcol)})
    for m in range(1, n_prow):
        pl.semaphore_signal(barrier, inc=1, device_id={"prow": partner(pr, m, n_prow)})

    row_ids = lax.broadcasted_iota(jnp.int32, (BR_DEV, LANES), 0)
    col_ids = lax.broadcasted_iota(jnp.int32, (col_blocks, LANES), 0)
    line = lax.broadcasted_iota(jnp.int32, (LANES, LANES), 0)
    for table, n in ((row_table, BR_DEV), (col_table, col_blocks)):
        turn = jnp.where(line < 3 * n, lax.rem(line, n), -2)
        turn = turn.astype(jnp.float32).astype(jnp.bfloat16)
        for i in range(n):
            table[i] = jnp.maximum(1.0 - jnp.abs(turn - float(i)), 0.0).astype(jnp.bfloat16)

    def lanes(h):
        return slice(h * LANES, (h + 1) * LANES)

    def widest(parts):
        while len(parts) > 1:
            pairs = [jnp.maximum(a, b) for a, b in zip(parts[::2], parts[1::2])]
            parts = pairs + parts[len(parts) - len(parts) % 2:]
        return parts[0]

    def keep(ref, s, h, top):
        ref[h, pl.ds(pl.multiple_of(s * SUB, SUB), SUB), :] = top

    def tops(ref, h, n):
        return widest([ref[h, pl.ds(k, n, stride=SUB), :] for k in range(SUB)])

    def first_tile(s):
        x = [[jnp.abs(block[s, g * PACK:(g + 1) * PACK, lanes(h)]) for h in range(halves)]
             for g in range(width // PACK)]
        for h in range(halves):
            top = widest([row[h] for row in x]).astype(jnp.float32)
            keep(col_slot, s, h, jnp.maximum(top[:SUB], top[SUB:]))
        fold = jnp.concatenate([widest(row) for row in x], axis=0).T
        top = widest([fold[k * PACK:(k + 1) * PACK] for k in range(LANES // PACK)])
        top = top.astype(jnp.float32)
        top = jnp.maximum(top[:SUB], top[SUB:])
        for h in range(halves):
            keep(row_slot, s, h, top[:, lanes(h)])

    def first_step(t, carry):
        load(t).wait()
        for j in range(STEP):
            first_tile(t * STEP + j)
        return carry

    def prepare(s, carry):
        x = jnp.abs(block[s])
        plain[s] = x.astype(jnp.float32)
        turned[s] = x.T.astype(jnp.float32)
        return carry

    def set_split(vec):
        n = vec.shape[0]
        top = vec.astype(jnp.bfloat16)
        left = vec - top.astype(jnp.float32)
        mid = left.astype(jnp.bfloat16)
        low = (left - mid.astype(jnp.float32)).astype(jnp.bfloat16)
        rest = jnp.zeros((LANES - 3 * n, width), jnp.bfloat16)
        stack = jnp.concatenate([top, mid, low, rest], axis=0)
        for h in range(halves):
            split[lanes(h), :] = stack[:, lanes(h)].T

    def spread_pair(ids_ref, table, p):
        pick = jnp.concatenate([table[ids_ref[2 * p + j]] for j in range(2)], axis=1)
        spread[p] = jnp.dot(split[...], pick, preferred_element_type=jnp.float32)

    def scale_tile(data, s, slot):
        best = [[None, None] for _ in range(halves)]
        for g in range(width // SUB):
            at = slice(g * SUB, (g + 1) * SUB)
            by = spread[s // 2, at, lanes(s % 2)]
            for h in range(halves):
                x = data[s, at, lanes(h)] * by
                old = best[h][g % 2]
                best[h][g % 2] = x if old is None else jnp.maximum(old, x)
        for h in range(halves):
            keep(slot, s, h, jnp.maximum(*best[h]))

    def one_pass(data, vec, ids_ref, slot):
        set_split(vec)
        table = row_table if ids_ref is brow_ref else col_table

        def run(n):
            pairs = n // 2
            for p in range(pairs + LEAD):
                if p < pairs:
                    spread_pair(ids_ref, table, p)
                if p >= LEAD:
                    for j in range(2):
                        scale_tile(data, 2 * (p - LEAD) + j, slot)

        @pl.when(holder)
        def _():
            run(slots)

        @pl.when(jnp.logical_not(holder))
        def _():
            run(few)

    def gather_slots(ref, kind, where_ids, n, out):
        for h in range(halves):
            slot_top[:n, lanes(h)] = tops(ref, h, n)
        acc = [jnp.zeros(where_ids.shape, jnp.float32) for _ in range(halves)]
        for s in range(n):
            hit = where_ids == own_ids[kind, s:s + 1, :]
            for h in range(halves):
                top = slot_top[s:s + 1, lanes(h)]
                acc[h] = jnp.maximum(acc[h], jnp.where(hit, top, 0.0))
        for h in range(halves):
            out[:, lanes(h)] = acc[h]

    def row_copies(k, rows):
        return [pltpu.make_async_remote_copy(
            src_ref=row_buf.at[k, pc, pl.ds(0, rows)], dst_ref=row_buf.at[k, pc, pl.ds(0, rows)],
            send_sem=row_send_sem.at[k, m - 1], recv_sem=row_recv_sem.at[k, pc],
            device_id={"pcol": partner(pc, m, n_pcol)},
        ) for m in range(n_pcol - 1, 0, -1)]

    def ids_copies():
        return [pltpu.make_async_remote_copy(
            src_ref=ids_row.at[pc], dst_ref=ids_row.at[pc],
            send_sem=ids_send_sem.at[m - 1], recv_sem=ids_recv_sem.at[pc],
            device_id={"pcol": partner(pc, m, n_pcol)},
        ) for m in range(n_pcol - 1, 0, -1)]

    def col_copies(k):
        return [pltpu.make_async_remote_copy(
            src_ref=col_buf.at[k, pr], dst_ref=col_buf.at[k, pr],
            send_sem=col_send_sem.at[k, m - 1], recv_sem=col_recv_sem.at[k, pr],
            device_id={"prow": partner(pr, m, n_prow)},
        ) for m in range(n_prow - 1, 0, -1)]

    def send_rows(k):
        @pl.when(holder)
        def _():
            gather_slots(row_slot, 1, row_ids, slots, row_buf.at[k, pc])
            for copy in row_copies(k, BR_DEV):
                copy.start()

        @pl.when(jnp.logical_not(holder))
        def _():
            for h in range(halves):
                row_buf[k, pc, :few, lanes(h)] = tops(row_slot, h, few)
            for copy in row_copies(k, few):
                copy.start()

    def send_cols(k):
        @pl.when(holder)
        def _():
            gather_slots(col_slot, 0, col_ids, slots, col_buf.at[k, pr])

        @pl.when(jnp.logical_not(holder))
        def _():
            gather_slots(col_slot, 0, col_ids, few, col_buf.at[k, pr])

        for copy in col_copies(k):
            copy.start()

    def arrived(copy):
        copy.wait_recv()

    per = n_pcol // group

    def place(i):
        return lax.rem(lax.rem(pr, group) + 1 + lax.div(i, per), group) + group * lax.rem(i, per)

    def wait_ids():
        for i in range(n_pcol - per):
            q = place(i)

            @pl.when(q != pc)
            def _():
                pltpu.make_async_remote_copy(
                    src_ref=ids_row.at[q], dst_ref=ids_row.at[q], send_sem=ids_send_sem.at[0],
                    recv_sem=ids_recv_sem.at[q], device_id={"pcol": q},
                ).wait_recv()

        for i in range(n_pcol - per):
            q = place(i)
            own = jnp.where(part == slot_of, jnp.broadcast_to(ids_row[q], (few, LANES)), -1)
            own = jnp.max(own.astype(jnp.float32), axis=1, keepdims=True)
            ids[q] = jnp.broadcast_to(own, (few, LANES)).astype(jnp.int32)

    def wait_rows(k):

        def wait_few(i):
            q = place(i)

            @pl.when(q != pc)
            def _():
                ref = row_buf.at[k, q, pl.ds(0, few)]
                pltpu.make_async_remote_copy(
                    src_ref=ref, dst_ref=ref, send_sem=row_send_sem.at[k, 0],
                    recv_sem=row_recv_sem.at[k, q], device_id={"pcol": q},
                ).wait_recv()

        def from_few(first, n, acc):
            for i in range(n):
                wait_few(first + i)
            acc = list(acc)
            for i in range(n):
                q = place(first + i)
                for s in range(few):
                    hit = row_ids == ids[q, s:s + 1, :]
                    for h in range(halves):
                        top = row_buf[k, q, s:s + 1, lanes(h)]
                        acc[h] = jnp.maximum(acc[h], jnp.where(hit, top, 0.0))
            return tuple(acc)

        zero = tuple(jnp.zeros((BR_DEV, LANES), jnp.float32) for _ in range(halves))
        rest, span = n_pcol - per, 3
        acc = lax.fori_loop(
            0, rest // span, lambda i, acc: from_few(i * span, span, acc), zero
        ) if rest > 2 * span else from_few(0, rest, zero)
        acc = jnp.concatenate(acc, axis=1)
        for i in range(per):
            q = lax.rem(pr, group) + group * i

            @pl.when(q != pc)
            def _():
                ref = row_buf.at[k, q]
                pltpu.make_async_remote_copy(
                    src_ref=ref, dst_ref=ref, send_sem=row_send_sem.at[k, 0],
                    recv_sem=row_recv_sem.at[k, q], device_id={"pcol": q},
                ).wait_recv()

            acc = jnp.maximum(acc, row_buf[k, q])
        return acc

    def wait_cols(k):
        for m in range(n_prow - 1, 0, -1):
            q = partner(pr, m, n_prow)
            ref = col_buf.at[k, q]
            pltpu.make_async_remote_copy(
                src_ref=ref, dst_ref=ref, send_sem=col_send_sem.at[k, m - 1],
                recv_sem=col_recv_sem.at[k, q], device_id={"prow": q},
            ).wait_recv()
        return widest([col_buf[k, q] for q in range(n_prow)])

    for meta in metas:
        meta.wait()
    for kind, ref in enumerate((bcol_ref, brow_ref)):
        for s in range(slots):
            own = jnp.where(s < count_ref[0], ref[s], -1)
            own_ids[kind, s:s + 1, :] = jnp.full((1, LANES), own, jnp.int32)
    part = lax.broadcasted_iota(jnp.int32, (few, LANES), 1) // (LANES // few)
    slot_of = lax.broadcasted_iota(jnp.int32, (few, LANES), 0)
    own = jnp.where(part == slot_of, own_ids[1, :few], -1)
    ids_row[pc] = jnp.max(own, axis=0, keepdims=True)
    peers = n_pcol - 1 + n_prow - 1

    @pl.when(holder)
    def _():
        lax.fori_loop(0, slots // STEP, first_step, 0)
        pl.semaphore_wait(barrier, peers)

    @pl.when(jnp.logical_not(holder))
    def _():
        lax.fori_loop(0, few // STEP // 2, first_step, 0)
        pl.semaphore_wait(barrier, peers)
        for copy in ids_copies():
            copy.start()
        lax.fori_loop(few // STEP // 2, few // STEP, first_step, 0)

    send_rows(0)
    send_cols(0)

    lax.fori_loop(0, steps * STEP, prepare, 0)

    wait_ids()
    one = jnp.ones((BR_DEV, width), jnp.float32)
    row_1 = rescale(one, wait_rows(0))
    one_pass(plain, row_1, brow_ref, col_slot)
    send_cols(1)
    col_1 = rescale(jnp.ones((col_blocks, width), jnp.float32), wait_cols(0))
    one_pass(turned, col_1 * LIFT, bcol_ref, row_slot)
    send_rows(1)
    row_vec[...] = row_1

    def scale_turned(s, carry):
        turned[s] = turned[s] * row_vec[pl.ds(brow_ref[s], 1), :]
        return carry

    lax.fori_loop(0, steps * STEP, scale_turned, 0)
    col_2 = rescale(col_1, col_1 * wait_cols(1))
    one_pass(turned, col_2, bcol_ref, row_slot)
    send_rows(2)
    row_max = (row_1 * wait_rows(1)) / LIFT
    row_2 = rescale(row_1, row_max)
    one_pass(plain, row_2, brow_ref, col_slot)
    send_cols(2)
    change = 1.0 / jnp.sqrt(row_max)
    row_out[...] = rescale(row_2, change * wait_rows(2))
    col_out[...] = rescale(col_2, col_2 * wait_cols(2))

    for k in range(SWEEPS):
        @pl.when(holder)
        def _():
            for copy in row_copies(k, BR_DEV):
                copy.wait_send()

        @pl.when(jnp.logical_not(holder))
        def _():
            for copy in row_copies(k, few):
                copy.wait_send()
            if k == 0:
                for copy in ids_copies():
                    copy.wait_send()

        for copy in col_copies(k):
            copy.wait_send()


def spell(row_ref, col_ref, row_out, col_out):
    for ref, out in ((row_ref, row_out), (col_ref, col_out)):
        for i in range(ref.shape[0]):
            out[i] = ref[i:i + 1, :]


def solution(mesh):
    n_prow, n_pcol = mesh.shape["prow"], mesh.shape["pcol"]

    def on_device(tiles, tile_brow, tile_bcol, tile_count):
        slots, width = tiles.shape[2], tiles.shape[3]
        col_blocks = BR_DEV * n_prow // n_pcol
        halves = width // LANES
        vmem = pl.BlockSpec(memory_space=pltpu.VMEM)
        anywhere = pl.BlockSpec(memory_space=pl.ANY)
        row_vec, col_vec = pl.pallas_call(
            functools.partial(kernel, n_prow, n_pcol, col_blocks, slots, width),
            out_shape=(
                jax.ShapeDtypeStruct((BR_DEV, width), jnp.float32),
                jax.ShapeDtypeStruct((col_blocks, width), jnp.float32),
            ),
            in_specs=[anywhere] * 4,
            out_specs=(vmem, vmem),
            scratch_shapes=[
                pltpu.SMEM((slots,), jnp.int32),
                pltpu.SMEM((slots,), jnp.int32),
                pltpu.SMEM((1,), jnp.int32),
                pltpu.VMEM((slots, width, width), jnp.bfloat16),
                pltpu.VMEM((slots, width, width), jnp.float32),
                pltpu.VMEM((slots, width, width), jnp.float32),
                pltpu.VMEM((halves, slots * SUB, LANES), jnp.float32),
                pltpu.VMEM((halves, slots * SUB, LANES), jnp.float32),
                pltpu.VMEM((width, LANES), jnp.bfloat16),
                pltpu.VMEM((slots // 2, width, 2 * LANES), jnp.float32),
                pltpu.VMEM((BR_DEV, LANES, LANES), jnp.bfloat16),
                pltpu.VMEM((col_blocks, LANES, LANES), jnp.bfloat16),
                pltpu.VMEM((BR_DEV, width), jnp.float32),
                pltpu.VMEM((slots, width), jnp.float32),
                pltpu.VMEM((2, slots, LANES), jnp.int32),
                pltpu.VMEM((n_pcol, 1, LANES), jnp.int32),
                pltpu.VMEM((n_pcol, slots // 2, LANES), jnp.int32),
                pltpu.VMEM((SWEEPS, n_pcol, BR_DEV, width), jnp.float32),
                pltpu.VMEM((SWEEPS, n_prow, col_blocks, width), jnp.float32),
                pltpu.SemaphoreType.DMA((3,)),
                pltpu.SemaphoreType.DMA((slots // STEP,)),
                pltpu.SemaphoreType.DMA((n_pcol - 1,)),
                pltpu.SemaphoreType.DMA((n_pcol,)),
                pltpu.SemaphoreType.DMA((SWEEPS, n_pcol - 1)),
                pltpu.SemaphoreType.DMA((SWEEPS, n_pcol)),
                pltpu.SemaphoreType.DMA((SWEEPS, n_prow - 1)),
                pltpu.SemaphoreType.DMA((SWEEPS, n_prow)),
            ],
            compiler_params=pltpu.CompilerParams(
                collective_id=0, has_side_effects=True, vmem_limit_bytes=53 << 20
            ),
        )(
            pltpu.with_memory_space_constraint(tile_brow.reshape(slots), pltpu.HBM),
            pltpu.with_memory_space_constraint(tile_bcol.reshape(slots), pltpu.HBM),
            tile_count.reshape(1),
            tiles.reshape(slots, width, width),
        )
        return pl.pallas_call(
            spell,
            out_shape=(
                jax.ShapeDtypeStruct((BR_DEV, 1, width), jnp.float32),
                jax.ShapeDtypeStruct((col_blocks, 1, width), jnp.float32),
            ),
            in_specs=[vmem, vmem],
            out_specs=(vmem, vmem),
            compiler_params=pltpu.CompilerParams(vmem_limit_bytes=4 << 20),
        )(row_vec, col_vec)

    return jax.shard_map(
        on_device,
        mesh=mesh,
        in_specs=(
            P("prow", "pcol", None, None, None),
            P("prow", "pcol", None),
            P("prow", "pcol", None),
            P("prow", "pcol"),
        ),
        out_specs=(P(None, "prow", None), P(None, "pcol", None)),
        check_vma=False,
    )
```

```python
import functools
import math

import jax
import jax.numpy as jnp
from jax import lax
from jax.experimental import pallas as pl
from jax.experimental.pallas import tpu as pltpu
from jax.sharding import PartitionSpec as P

BR_DEV = 32
SWEEPS = 3
LANES = 128
SUB = 8
STEP = 4
PACK = 16
LEAD = 2
LIFT = 2.0 ** 63


def rescale(scale, largest):
    return scale / jnp.sqrt(largest)


def partner(at, mask, size):
    out, bit = at, 1
    while bit < size:
        if mask & bit:
            out = out + bit * (1 - 2 * lax.rem(lax.div(at, bit), 2))
        bit *= 2
    return out


def kernel(
    n_prow, n_pcol, col_blocks, slots, width,
    brow_hbm, bcol_hbm, count_hbm, tiles_ref,
    row_out, col_out,
    brow_ref, bcol_ref, count_ref,
    block, plain, turned, row_slot, col_slot, split, spread, row_table, col_table, row_vec, slot_top, own_ids,
    ids_row, ids, row_buf, col_buf,
    meta_sem, load_sem, ids_send_sem, ids_recv_sem,
    row_send_sem, row_recv_sem, col_send_sem, col_recv_sem,
):
    halves = width // LANES
    group = math.gcd(n_prow, n_pcol)
    few = slots // 2
    pr = lax.axis_index("prow")
    pc = lax.axis_index("pcol")
    holder = lax.rem(pc, group) == lax.rem(pr, group)
    steps = jnp.where(holder, slots, few) // STEP

    def load(t):
        at = pl.ds(t * STEP, STEP)
        return pltpu.make_async_copy(tiles_ref.at[at], block.at[at], load_sem.at[t])

    for t in range(few // STEP):
        load(t).start()

    @pl.when(holder)
    def _():
        for t in range(few // STEP, slots // STEP):
            load(t).start()

    metas = [
        pltpu.make_async_copy(brow_hbm, brow_ref, meta_sem.at[0]),
        pltpu.make_async_copy(bcol_hbm, bcol_ref, meta_sem.at[1]),
        pltpu.make_async_copy(count_hbm, count_ref, meta_sem.at[2]),
    ]
    for meta in metas:
        meta.start()
    barrier = pltpu.get_barrier_semaphore()
    for m in range(1, n_pcol):
        pl.semaphore_signal(barrier, inc=1, device_id={"pcol": partner(pc, m, n_pcol)})
    for m in range(1, n_prow):
        pl.semaphore_signal(barrier, inc=1, device_id={"prow": partner(pr, m, n_prow)})

    row_ids = lax.broadcasted_iota(jnp.int32, (BR_DEV, LANES), 0)
    col_ids = lax.broadcasted_iota(jnp.int32, (col_blocks, LANES), 0)
    line = lax.broadcasted_iota(jnp.int32, (LANES, LANES), 0)
    for table, n in ((row_table, BR_DEV), (col_table, col_blocks)):
        turn = jnp.where(line < 3 * n, lax.rem(line, n), -2)
        turn = turn.astype(jnp.float32).astype(jnp.bfloat16)
        for i in range(n):
            table[i] = jnp.maximum(1.0 - jnp.abs(turn - float(i)), 0.0).astype(jnp.bfloat16)

    def lanes(h):
        return slice(h * LANES, (h + 1) * LANES)

    def widest(parts):
        while len(parts) > 1:
            pairs = [jnp.maximum(a, b) for a, b in zip(parts[::2], parts[1::2])]
            parts = pairs + parts[len(parts) - len(parts) % 2:]
        return parts[0]

    def keep(ref, s, h, top):
        ref[h, pl.ds(pl.multiple_of(s * SUB, SUB), SUB), :] = top

    def tops(ref, h, n):
        return widest([ref[h, pl.ds(k, n, stride=SUB), :] for k in range(SUB)])

    def first_tile(s):
        x = [[jnp.abs(block[s, g * PACK:(g + 1) * PACK, lanes(h)]) for h in range(halves)]
             for g in range(width // PACK)]
        for h in range(halves):
            top = widest([row[h] for row in x]).astype(jnp.float32)
            keep(col_slot, s, h, jnp.maximum(top[:SUB], top[SUB:]))
        fold = jnp.concatenate([widest(row) for row in x], axis=0).T
        top = widest([fold[k * PACK:(k + 1) * PACK] for k in range(LANES // PACK)])
        top = top.astype(jnp.float32)
        top = jnp.maximum(top[:SUB], top[SUB:])
        for h in range(halves):
            keep(row_slot, s, h, top[:, lanes(h)])

    def first_step(t, carry):
        load(t).wait()
        for j in range(STEP):
            first_tile(t * STEP + j)
        return carry

    def prepare(s, carry):
        x = jnp.abs(block[s])
        plain[s] = x.astype(jnp.float32)
        turned[s] = x.T.astype(jnp.float32)
        return carry

    def set_split(vec):
        n = vec.shape[0]
        top = vec.astype(jnp.bfloat16)
        left = vec - top.astype(jnp.float32)
        mid = left.astype(jnp.bfloat16)
        low = (left - mid.astype(jnp.float32)).astype(jnp.bfloat16)
        rest = jnp.zeros((LANES - 3 * n, width), jnp.bfloat16)
        stack = jnp.concatenate([top, mid, low, rest], axis=0)
        for h in range(halves):
            split[lanes(h), :] = stack[:, lanes(h)].T

    def spread_pair(ids_ref, table, p):
        pick = jnp.concatenate([table[ids_ref[2 * p + j]] for j in range(2)], axis=1)
        spread[p] = jnp.dot(split[...], pick, preferred_element_type=jnp.float32)

    def scale_tile(data, s, slot):
        best = [[None, None] for _ in range(halves)]
        for g in range(width // SUB):
            at = slice(g * SUB, (g + 1) * SUB)
            by = spread[s // 2, at, lanes(s % 2)]
            for h in range(halves):
                x = data[s, at, lanes(h)] * by
                old = best[h][g % 2]
                best[h][g % 2] = x if old is None else jnp.maximum(old, x)
        for h in range(halves):
            keep(slot, s, h, jnp.maximum(*best[h]))

    def one_pass(data, vec, ids_ref, slot):
        set_split(vec)
        table = row_table if ids_ref is brow_ref else col_table

        def run(n):
            pairs = n // 2
            for p in range(pairs + LEAD):
                if p < pairs:
                    spread_pair(ids_ref, table, p)
                if p >= LEAD:
                    for j in range(2):
                        scale_tile(data, 2 * (p - LEAD) + j, slot)

        @pl.when(holder)
        def _():
            run(slots)

        @pl.when(jnp.logical_not(holder))
        def _():
            run(few)

    def gather_slots(ref, kind, where_ids, n, out):
        for h in range(halves):
            slot_top[:n, lanes(h)] = tops(ref, h, n)
        acc = [jnp.zeros(where_ids.shape, jnp.float32) for _ in range(halves)]
        for s in range(n):
            hit = where_ids == own_ids[kind, s:s + 1, :]
            for h in range(halves):
                top = slot_top[s:s + 1, lanes(h)]
                acc[h] = jnp.maximum(acc[h], jnp.where(hit, top, 0.0))
        for h in range(halves):
            out[:, lanes(h)] = acc[h]

    def row_copies(k, rows):
        return [pltpu.make_async_remote_copy(
            src_ref=row_buf.at[k, pc, pl.ds(0, rows)], dst_ref=row_buf.at[k, pc, pl.ds(0, rows)],
            send_sem=row_send_sem.at[k, m - 1], recv_sem=row_recv_sem.at[k, pc],
            device_id={"pcol": partner(pc, m, n_pcol)},
        ) for m in range(n_pcol - 1, 0, -1)]

    def ids_copies():
        return [pltpu.make_async_remote_copy(
            src_ref=ids_row.at[pc], dst_ref=ids_row.at[pc],
            send_sem=ids_send_sem.at[m - 1], recv_sem=ids_recv_sem.at[pc],
            device_id={"pcol": partner(pc, m, n_pcol)},
        ) for m in range(n_pcol - 1, 0, -1)]

    def col_copies(k):
        return [pltpu.make_async_remote_copy(
            src_ref=col_buf.at[k, pr], dst_ref=col_buf.at[k, pr],
            send_sem=col_send_sem.at[k, m - 1], recv_sem=col_recv_sem.at[k, pr],
            device_id={"prow": partner(pr, m, n_prow)},
        ) for m in range(n_prow - 1, 0, -1)]

    def send_rows(k):
        @pl.when(holder)
        def _():
            gather_slots(row_slot, 1, row_ids, slots, row_buf.at[k, pc])
            for copy in row_copies(k, BR_DEV):
                copy.start()

        @pl.when(jnp.logical_not(holder))
        def _():
            for h in range(halves):
                row_buf[k, pc, :few, lanes(h)] = tops(row_slot, h, few)
            for copy in row_copies(k, few):
                copy.start()

    def send_cols(k):
        @pl.when(holder)
        def _():
            gather_slots(col_slot, 0, col_ids, slots, col_buf.at[k, pr])

        @pl.when(jnp.logical_not(holder))
        def _():
            gather_slots(col_slot, 0, col_ids, few, col_buf.at[k, pr])

        for copy in col_copies(k):
            copy.start()

    def arrived(copy):
        copy.wait_recv()

    per = n_pcol // group

    def place(i):
        return lax.rem(lax.rem(pr, group) + 1 + lax.div(i, per), group) + group * lax.rem(i, per)

    def wait_ids():
        for i in range(n_pcol - per):
            q = place(i)

            @pl.when(q != pc)
            def _():
                pltpu.make_async_remote_copy(
                    src_ref=ids_row.at[q], dst_ref=ids_row.at[q], send_sem=ids_send_sem.at[0],
                    recv_sem=ids_recv_sem.at[q], device_id={"pcol": q},
                ).wait_recv()

        for i in range(n_pcol - per):
            q = place(i)
            own = jnp.where(part == slot_of, jnp.broadcast_to(ids_row[q], (few, LANES)), -1)
            own = jnp.max(own.astype(jnp.float32), axis=1, keepdims=True)
            ids[q] = jnp.broadcast_to(own, (few, LANES)).astype(jnp.int32)

    def wait_rows(k):

        def wait_few(i):
            q = place(i)

            @pl.when(q != pc)
            def _():
                ref = row_buf.at[k, q, pl.ds(0, few)]
                pltpu.make_async_remote_copy(
                    src_ref=ref, dst_ref=ref, send_sem=row_send_sem.at[k, 0],
                    recv_sem=row_recv_sem.at[k, q], device_id={"pcol": q},
                ).wait_recv()

        def from_few(first, n, acc):
            for i in range(n):
                wait_few(first + i)
            acc = list(acc)
            for i in range(n):
                q = place(first + i)
                for s in range(few):
                    hit = row_ids == ids[q, s:s + 1, :]
                    for h in range(halves):
                        top = row_buf[k, q, s:s + 1, lanes(h)]
                        acc[h] = jnp.maximum(acc[h], jnp.where(hit, top, 0.0))
            return tuple(acc)

        zero = tuple(jnp.zeros((BR_DEV, LANES), jnp.float32) for _ in range(halves))
        rest, span = n_pcol - per, 3
        acc = lax.fori_loop(
            0, rest // span, lambda i, acc: from_few(i * span, span, acc), zero
        ) if rest > 2 * span else from_few(0, rest, zero)
        acc = jnp.concatenate(acc, axis=1)
        for i in range(per):
            q = lax.rem(pr, group) + group * i

            @pl.when(q != pc)
            def _():
                ref = row_buf.at[k, q]
                pltpu.make_async_remote_copy(
                    src_ref=ref, dst_ref=ref, send_sem=row_send_sem.at[k, 0],
                    recv_sem=row_recv_sem.at[k, q], device_id={"pcol": q},
                ).wait_recv()

            acc = jnp.maximum(acc, row_buf[k, q])
        return acc

    def wait_cols(k):
        for m in range(n_prow - 1, 0, -1):
            q = partner(pr, m, n_prow)
            ref = col_buf.at[k, q]
            pltpu.make_async_remote_copy(
                src_ref=ref, dst_ref=ref, send_sem=col_send_sem.at[k, m - 1],
                recv_sem=col_recv_sem.at[k, q], device_id={"prow": q},
            ).wait_recv()
        return widest([col_buf[k, q] for q in range(n_prow)])

    def sent(k):
        @pl.when(holder)
        def _():
            for copy in row_copies(k, BR_DEV):
                copy.wait_send()

        @pl.when(jnp.logical_not(holder))
        def _():
            for copy in row_copies(k, few):
                copy.wait_send()
            if k == 0:
                for copy in ids_copies():
                    copy.wait_send()

        for copy in col_copies(k):
            copy.wait_send()

    for meta in metas:
        meta.wait()
    for kind, ref in enumerate((bcol_ref, brow_ref)):
        for s in range(slots):
            own = jnp.where(s < count_ref[0], ref[s], -1)
            own_ids[kind, s:s + 1, :] = jnp.full((1, LANES), own, jnp.int32)
    part = lax.broadcasted_iota(jnp.int32, (few, LANES), 1) // (LANES // few)
    slot_of = lax.broadcasted_iota(jnp.int32, (few, LANES), 0)
    own = jnp.where(part == slot_of, own_ids[1, :few], -1)
    ids_row[pc] = jnp.max(own, axis=0, keepdims=True)
    peers = n_pcol - 1 + n_prow - 1

    @pl.when(holder)
    def _():
        lax.fori_loop(0, slots // STEP, first_step, 0)
        pl.semaphore_wait(barrier, peers)

    @pl.when(jnp.logical_not(holder))
    def _():
        lax.fori_loop(0, few // STEP // 2, first_step, 0)
        pl.semaphore_wait(barrier, peers)
        for copy in ids_copies():
            copy.start()
        lax.fori_loop(few // STEP // 2, few // STEP, first_step, 0)

    send_cols(0)
    send_rows(0)

    lax.fori_loop(0, steps * STEP, prepare, 0)

    wait_ids()
    one = jnp.ones((BR_DEV, width), jnp.float32)
    row_1 = rescale(one, wait_rows(0))
    one_pass(plain, row_1, brow_ref, col_slot)
    send_cols(1)
    col_1 = rescale(jnp.ones((col_blocks, width), jnp.float32), wait_cols(0))
    one_pass(turned, col_1 * LIFT, bcol_ref, row_slot)
    send_rows(1)
    row_vec[...] = row_1

    def scale_turned(s, carry):
        turned[s] = turned[s] * row_vec[pl.ds(brow_ref[s], 1), :]
        return carry

    lax.fori_loop(0, steps * STEP, scale_turned, 0)
    sent(0)
    col_2 = rescale(col_1, col_1 * wait_cols(1))
    one_pass(turned, col_2, bcol_ref, row_slot)
    send_rows(2)
    row_max = (row_1 * wait_rows(1)) / LIFT
    row_2 = rescale(row_1, row_max)
    one_pass(plain, row_2, brow_ref, col_slot)
    send_cols(2)
    for k in range(1, SWEEPS):
        sent(k)
    change = 1.0 / jnp.sqrt(row_max)
    row_out[...] = rescale(row_2, change * wait_rows(2))
    col_out[...] = rescale(col_2, col_2 * wait_cols(2))


def spell(row_ref, col_ref, row_out, col_out):
    for ref, out in ((row_ref, row_out), (col_ref, col_out)):
        for i in range(ref.shape[0]):
            out[i] = ref[i:i + 1, :]


def solution(mesh):
    n_prow, n_pcol = mesh.shape["prow"], mesh.shape["pcol"]

    def on_device(tiles, tile_brow, tile_bcol, tile_count):
        slots, width = tiles.shape[2], tiles.shape[3]
        col_blocks = BR_DEV * n_prow // n_pcol
        halves = width // LANES
        vmem = pl.BlockSpec(memory_space=pltpu.VMEM)
        anywhere = pl.BlockSpec(memory_space=pl.ANY)
        row_vec, col_vec = pl.pallas_call(
            functools.partial(kernel, n_prow, n_pcol, col_blocks, slots, width),
            out_shape=(
                jax.ShapeDtypeStruct((BR_DEV, width), jnp.float32),
                jax.ShapeDtypeStruct((col_blocks, width), jnp.float32),
            ),
            in_specs=[anywhere] * 4,
            out_specs=(vmem, vmem),
            scratch_shapes=[
                pltpu.SMEM((slots,), jnp.int32),
                pltpu.SMEM((slots,), jnp.int32),
                pltpu.SMEM((1,), jnp.int32),
                pltpu.VMEM((slots, width, width), jnp.bfloat16),
                pltpu.VMEM((slots, width, width), jnp.float32),
                pltpu.VMEM((slots, width, width), jnp.float32),
                pltpu.VMEM((halves, slots * SUB, LANES), jnp.float32),
                pltpu.VMEM((halves, slots * SUB, LANES), jnp.float32),
                pltpu.VMEM((width, LANES), jnp.bfloat16),
                pltpu.VMEM((slots // 2, width, 2 * LANES), jnp.float32),
                pltpu.VMEM((BR_DEV, LANES, LANES), jnp.bfloat16),
                pltpu.VMEM((col_blocks, LANES, LANES), jnp.bfloat16),
                pltpu.VMEM((BR_DEV, width), jnp.float32),
                pltpu.VMEM((slots, width), jnp.float32),
                pltpu.VMEM((2, slots, LANES), jnp.int32),
                pltpu.VMEM((n_pcol, 1, LANES), jnp.int32),
                pltpu.VMEM((n_pcol, slots // 2, LANES), jnp.int32),
                pltpu.VMEM((SWEEPS, n_pcol, BR_DEV, width), jnp.float32),
                pltpu.VMEM((SWEEPS, n_prow, col_blocks, width), jnp.float32),
                pltpu.SemaphoreType.DMA((3,)),
                pltpu.SemaphoreType.DMA((slots // STEP,)),
                pltpu.SemaphoreType.DMA((n_pcol - 1,)),
                pltpu.SemaphoreType.DMA((n_pcol,)),
                pltpu.SemaphoreType.DMA((SWEEPS, n_pcol - 1)),
                pltpu.SemaphoreType.DMA((SWEEPS, n_pcol)),
                pltpu.SemaphoreType.DMA((SWEEPS, n_prow - 1)),
                pltpu.SemaphoreType.DMA((SWEEPS, n_prow)),
            ],
            compiler_params=pltpu.CompilerParams(
                collective_id=0, has_side_effects=True, vmem_limit_bytes=53 << 20
            ),
        )(
            pltpu.with_memory_space_constraint(tile_brow.reshape(slots), pltpu.HBM),
            pltpu.with_memory_space_constraint(tile_bcol.reshape(slots), pltpu.HBM),
            tile_count.reshape(1),
            tiles.reshape(slots, width, width),
        )
        return pl.pallas_call(
            spell,
            out_shape=(
                jax.ShapeDtypeStruct((BR_DEV, 1, width), jnp.float32),
                jax.ShapeDtypeStruct((col_blocks, 1, width), jnp.float32),
            ),
            in_specs=[vmem, vmem],
            out_specs=(vmem, vmem),
            compiler_params=pltpu.CompilerParams(vmem_limit_bytes=4 << 20),
        )(row_vec, col_vec)

    return jax.shard_map(
        on_device,
        mesh=mesh,
        in_specs=(
            P("prow", "pcol", None, None, None),
            P("prow", "pcol", None),
            P("prow", "pcol", None),
            P("prow", "pcol"),
        ),
        out_specs=(P(None, "prow", None), P(None, "pcol", None)),
        check_vma=False,
    )
```
